32 devices in a mesh: grp: 8 (over z, y), tp: 4 (over x, core).
Axes of the slice: x: 2, y: 2, z: 4, core: 2. Of those that a mesh axis runs over, the one named last changes fastest.
Arguments:
- source_rows: bfloat16 [4096, 2048], P('grp', 'tp'), may hold values from -0.09375 to 0.09375
- span_order: int32 [8], replicated, may hold values from 0 to 7, each once
- head_map: int32 [8], replicated, may hold values from 0 to 7, as said below
Outputs:
- packed: float32 [2048, 4096], P('tp')
The draws below stay inside these ranges and needn't reach their ends.
Inputs may be any that keep to these rules, and one draw needn't show every extreme that they name: `span_order`: a permutation of the 8 row blocks. `head_map`: a permutation of the 8 heads in which slot i of serving shard s takes a head of trainer shard (s + 2 + i) mod 4, trainer shard k holding heads k * 2 to k * 2 + 1.
All inputs are finite; a program needn't handle non-finite values.
Results may differ from the reference program's by a relative error of at most 0.0003.
Values may be sent and summed in bfloat16 or wider, within the bound.
A program may use at most 64 MiB of HBM per device.

```python
import jax
import jax.numpy as jnp

DW = 4096
KVH = 8
HD = 128
BLOCKS = 8
N_GRP = 8
N_TP = 4


def draw_head_map(key, part):
    per_shard = KVH // N_TP
    slots = jnp.arange(KVH, dtype=jnp.int32)
    serving = slots // per_shard
    within = slots % per_shard
    source = (serving + N_TP // 2 + within) % N_TP
    rotation = jax.random.randint(jax.random.fold_in(key, 17), (N_TP,), 0, per_shard).astype(jnp.int32)
    position = (within + jnp.take(rotation, source)) % per_shard
    return (source * per_shard + position).astype(jnp.int32)


def shard_levels(key, shape, shards, low, top_value):
    loudness = 1.0
    for axis_at, shards_of in shards:
        heights = jax.random.uniform(jax.random.fold_in(jax.random.fold_in(key, 6), axis_at), (shards_of,), jnp.float32, low / len(shards), top_value / len(shards))
        loudness = loudness * jnp.repeat(jnp.exp(heights), shape[axis_at] // shards_of).reshape((-1,) + (1,) * (len(shape) - 1 - axis_at))
    return loudness


def normal_values(stream_key, extent, width, reach, pieces=(), kind=jnp.bfloat16):
    result = jax.random.normal(stream_key, extent, jnp.float32) * width
    if len(pieces) > 0:
        result = shard_levels(stream_key, extent, pieces, -0.22, 0.18) * result
    return jnp.clip(result, min=-reach, max=reach).astype(kind)


def setup_inputs(seed: int = 0) -> dict:
    arg_keys = jax.random.split(jax.random.key(seed), 4)
    source_rows = normal_values(arg_keys[0], (DW, 2 * KVH * HD), DW ** -0.5, 0.09375, ((0, 8), (1, 4)))
    span_order = jax.random.permutation(arg_keys[1], BLOCKS).astype(jnp.int32)
    head_map = draw_head_map(jax.random.fold_in(arg_keys[3], 71), 0)
    return {"source_rows": source_rows, "span_order": span_order, "head_map": head_map}


def reference(source_rows, span_order, head_map):
    block_count = N_GRP
    row_count = DW // block_count
    inverse = jnp.zeros((block_count,), jnp.int32).at[span_order].set(jnp.arange(block_count, dtype=jnp.int32))
    weight = source_rows.reshape(block_count, row_count, 2 * KVH * HD)[inverse].reshape(DW, KVH, 2, HD)
    chosen = weight[:, head_map]
    chosen = chosen.reshape(DW, N_TP, KVH // N_TP, 2, HD).transpose(1, 3, 2, 4, 0)
    return chosen.reshape(2 * KVH * HD, DW).astype(jnp.float32)
```

```python
import functools

import jax
import jax.numpy as jnp
from jax import lax
from jax.experimental import pallas as pl
from jax.experimental.pallas import tpu as pltpu
from jax.sharding import PartitionSpec as P

MESH = pl.DeviceIdType.MESH
CHUNKS = 2


def ring_member(position, n):
    half = position // (n // 2)
    return 2 * position * (1 - half) + (2 * (n - 1 - position) + 1) * half


def ring_position(member, n):
    odd = member % 2
    return (member // 2) * (1 - odd) + (n - 1 - member // 2) * odd


def gather_kernel(n, tp, pieces, gathered, x_send, x_recv, r_send, r_recv):
    slots, rows = pieces.shape[0], pieces.shape[1]
    me, k = lax.axis_index("grp"), lax.axis_index("tp")
    position = ring_position(me, n)
    ring = [ring_member((position + 1) % n, n), ring_member((position + n - 1) % n, n)]
    size = rows // (2 * CHUNKS)
    parts = [(c, i) for c in range(CHUNKS) for i in reversed(range(slots))]

    barrier = pltpu.get_barrier_semaphore()
    for step in range(1, tp):
        pl.semaphore_signal(barrier, inc=1, device_id=(me, (k + step) % tp), device_id_type=MESH)
    for other in ring:
        pl.semaphore_signal(barrier, inc=1, device_id=(other, k), device_id_type=MESH)
    pl.semaphore_wait(barrier, tp + 1)

    def exchange(at, way):
        c, i = parts[at]
        span = pl.ds((way * CHUNKS + c) * size, size)
        return pltpu.make_async_remote_copy(
            src_ref=pieces.at[i, span],
            dst_ref=gathered.at[me, i, span],
            send_sem=x_send.at[way, at],
            recv_sem=x_recv.at[way, at],
            device_id=(me, (k + 2 * tp - tp // 2 - i) % tp),
            device_id_type=MESH,
        )

    def hop(step, at, way):
        c, i = parts[at]
        span = pl.ds((way * CHUNKS + c) * size, size)
        owner = ring_member((position + (n - step if way == 0 else step)) % n, n)
        return pltpu.make_async_remote_copy(
            src_ref=gathered.at[owner, i, span],
            dst_ref=gathered.at[owner, i, span],
            send_sem=r_send.at[step, way, at],
            recv_sem=r_recv.at[step, way, at],
            device_id=(ring[way], k),
            device_id_type=MESH,
        )

    for at in range(len(parts)):
        for way in range(2):
            exchange(at, way).start()
    for at in range(len(parts)):
        for way in range(2):
            exchange(at, way).wait_recv()
            hop(0, at, way).start()

    def forward(step, carry):
        for at in range(len(parts)):
            for way in range(2):
                hop(step - 1, at, way).wait_recv()
                hop(step, at, way).start()
        return carry

    lax.fori_loop(1, n - 1, forward, 0)
    for at in range(len(parts)):
        for way in range(2):
            hop(n - 2, at, way).wait_recv()
            exchange(at, way).wait_send()

    def drain(step, carry):
        for at in range(len(parts)):
            for way in range(2):
                hop(step, at, way).wait_send()
        return carry

    lax.fori_loop(0, n - 1, drain, 0)


def pack_kernel(inverse, *refs):
    blocks, out = refs[:-1], refs[-1]
    slots, width = blocks[0].shape[1], blocks[0].shape[3] // 2
    for c in range(2):
        for i in range(slots):
            cut = [b[0, i, :, c * width:(c + 1) * width].astype(jnp.float32) for b in blocks]
            whole = cut[0] if len(cut) == 1 else jnp.concatenate(cut, axis=0)
            out[pl.ds((c * slots + i) * width, width), :] = whole.T


def invert_order(span_order):
    block_count = span_order.shape[0]
    positions = jnp.arange(block_count, dtype=jnp.int32)
    matches = (span_order[:, None] == positions[None, :]).astype(jnp.int32)
    return jnp.sum(matches * positions[:, None], axis=0)


def local(n, tp, source_rows, span_order, head_map):
    rows = source_rows.shape[0]
    slots = head_map.shape[0] // tp
    columns = source_rows.shape[1] // slots
    k = lax.axis_index("tp")
    heads = source_rows.reshape(rows, slots, columns)
    pieces = []
    for i in range(slots):
        served = lax.rem(k + 2 * tp - tp // 2 - i, tp)
        head = lax.dynamic_index_in_dim(head_map, served * slots + i, keepdims=False) - k * slots
        pieces.append(lax.dynamic_index_in_dim(heads, head, axis=1, keepdims=False))
    pieces = jnp.stack(pieces)
    parts = CHUNKS * slots
    gathered = pl.pallas_call(
        functools.partial(gather_kernel, n, tp),
        out_shape=jax.ShapeDtypeStruct((n, slots, rows, columns), source_rows.dtype),
        in_specs=[pl.BlockSpec(memory_space=pl.ANY)],
        out_specs=pl.BlockSpec(memory_space=pl.ANY),
        scratch_shapes=[
            pltpu.SemaphoreType.DMA((2, parts)),
            pltpu.SemaphoreType.DMA((2, parts)),
            pltpu.SemaphoreType.DMA((n - 1, 2, parts)),
            pltpu.SemaphoreType.DMA((n - 1, 2, parts)),
        ],
        compiler_params=pltpu.CompilerParams(
            collective_id=0, has_side_effects=True, vmem_limit_bytes=8 * 1024 * 1024
        ),
        name="gather",
    )(pieces)
    inverse = invert_order(span_order)
    together = max(1, 128 // rows)
    packed = pl.pallas_call(
        pack_kernel,
        out_shape=jax.ShapeDtypeStruct((slots * columns, n * rows), jnp.float32),
        grid_spec=pltpu.PrefetchScalarGridSpec(
            num_scalar_prefetch=1,
            grid=(n // together,),
            in_specs=[
                pl.BlockSpec(
                    (1, slots, rows, columns),
                    functools.partial(lambda j, b, inv: (inv[b * together + j], 0, 0, 0), j),
                )
                for j in range(together)
            ],
            out_specs=pl.BlockSpec((slots * columns, together * rows), lambda b, inv: (0, b)),
        ),
        compiler_params=pltpu.CompilerParams(vmem_limit_bytes=16 * 1024 * 1024),
        name="pack",
    )(inverse, *[gathered] * together)
    return packed


def solution(mesh):
    n, tp = mesh.shape["grp"], mesh.shape["tp"]
    placed = (P("grp", "tp"), P(), P())
    return jax.shard_map(
        functools.partial(local, n, tp), mesh=mesh, in_specs=placed,
        out_specs=P("tp", None), check_vma=False,
    )
```

```python
import functools

import jax
import jax.numpy as jnp
from jax import lax
from jax.experimental import pallas as pl
from jax.experimental.pallas import tpu as pltpu
from jax.sharding import PartitionSpec as P

MESH = pl.DeviceIdType.MESH
CHUNKS = 2


def ring_member(position, n):
    half = position // (n // 2)
    return 2 * position * (1 - half) + (2 * (n - 1 - position) + 1) * half


def ring_position(member, n):
    odd = member % 2
    return (member // 2) * (1 - odd) + (n - 1 - member // 2) * odd


def pick_kernel(head_map, source, picked):
    picked[0] = source[...]


def gather_kernel(n, tp, pieces, gathered, carried, x_send, x_recv, r_send, r_recv, d_send, d_recv, o_send, o_recv):
    rows = pieces.shape[1]
    me, k = lax.axis_index("grp"), lax.axis_index("tp")
    position = ring_position(me, n)
    ring = [ring_member((position + 1) % n, n), ring_member((position + n - 1) % n, n)]
    size = rows // (2 * CHUNKS)
    every = [(c, way) for c in range(CHUNKS) for way in range(2)]
    served = [(k + 2 * tp - tp // 2 - i) % tp for i in range(2)]

    barrier = pltpu.get_barrier_semaphore()
    for step in range(1, tp):
        pl.semaphore_signal(barrier, inc=1, device_id=(me, (k + step) % tp), device_id_type=MESH)
    for other in ring:
        pl.semaphore_signal(barrier, inc=1, device_id=(other, k), device_id_type=MESH)
    pl.semaphore_wait(barrier, tp + 1)

    def span(c, way):
        return pl.ds((way * CHUNKS + c) * size, size)

    def send(src, dst, send_sem, recv_sem, to):
        return pltpu.make_async_remote_copy(
            src_ref=src, dst_ref=dst, send_sem=send_sem, recv_sem=recv_sem,
            device_id=to, device_id_type=MESH,
        )

    def held(step, way):
        return ring_member((position + (n - step if way == 0 else step)) % n, n)

    def exchange(c, way):
        return send(pieces.at[0, span(c, way)], gathered.at[me, 0, span(c, way)],
                    x_send.at[way, c], x_recv.at[way, c], (me, served[0]))

    def own(c, way):
        return send(pieces.at[1, span(c, way)], gathered.at[me, 1, span(c, way)],
                    o_send.at[way, c], o_recv.at[way, c], (me, served[1]))

    def hop(step, c, way):
        chunk = gathered.at[held(step, way), 0, span(c, way)]
        return send(chunk, chunk, r_send.at[step, way, c], r_recv.at[step, way, c], (ring[way], k))

    def first(c, way):
        return send(pieces.at[1, span(c, way)], carried.at[me, span(c, way)],
                    r_send.at[0, way, CHUNKS + c], r_recv.at[0, way, CHUNKS + c], (ring[way], k))

    def carry(step, c, way):
        chunk = carried.at[held(step, way), span(c, way)]
        return send(chunk, chunk, r_send.at[step, way, CHUNKS + c], r_recv.at[step, way, CHUNKS + c],
                    (ring[way], k))

    def hand(step, c, way):
        owner = held(step, way)
        return send(carried.at[owner, span(c, way)], gathered.at[owner, 1, span(c, way)],
                    d_send.at[step - 1, way, c], d_recv.at[step - 1, way, c], (me, served[1]))

    for c, way in every:
        exchange(c, way).start()
    for c, way in every:
        first(c, way).start()
    for c, way in every:
        exchange(c, way).wait_recv()
        hop(0, c, way).start()
    for c, way in every:
        own(c, way).start()

    def forward(step, _):
        for c, way in every:
            carry(step - 1, c, way).wait_recv()
            carry(step, c, way).start()
            hand(step, c, way).start()
        for c, way in every:
            hop(step - 1, c, way).wait_recv()
            hop(step, c, way).start()
        return _

    lax.fori_loop(1, n - 1, forward, 0)
    for c, way in every:
        carry(n - 2, c, way).wait_recv()
        hand(n - 1, c, way).start()
    for c, way in every:
        own(c, way).wait()
        exchange(c, way).wait_send()

    def drain(step, _):
        for c, way in every:
            hop(step, c, way).wait_send()
            carry(step, c, way).wait_send()
            hand(step + 1, c, way).wait()
        return _

    lax.fori_loop(0, n - 2, drain, 0)
    for c, way in every:
        hop(n - 2, c, way).wait_recv()
    drain(n - 2, 0)


def pack_kernel(order, *refs):
    blocks, out = refs[:-1], refs[-1]
    slots, width = blocks[0].shape[1], blocks[0].shape[3] // 2
    for c in range(2):
        for i in range(slots):
            cut = [b[0, i, :, c * width:(c + 1) * width] for b in blocks]
            whole = cut[0] if len(cut) == 1 else jnp.concatenate(cut, axis=0)
            out[pl.ds((c * slots + i) * width, width), :] = whole.T.astype(jnp.float32)


def invert_order(span_order):
    block_count = span_order.shape[0]
    positions = jnp.arange(block_count, dtype=jnp.int32)
    matches = (span_order[:, None] == positions[None, :]).astype(jnp.int32)
    return jnp.sum(matches * positions[:, None], axis=0)


def local(n, tp, source_rows, span_order, head_map):
    rows = source_rows.shape[0]
    slots = head_map.shape[0] // tp
    columns = source_rows.shape[1] // slots

    def head(i, head_map):
        k = lax.axis_index("tp")
        served = lax.rem(k + 2 * tp - tp // 2 - i, tp)
        return 0, head_map[served * slots + i] - k * slots

    pieces = pl.pallas_call(
        pick_kernel,
        out_shape=jax.ShapeDtypeStruct((slots, rows, columns), source_rows.dtype),
        grid_spec=pltpu.PrefetchScalarGridSpec(
            num_scalar_prefetch=1,
            grid=(slots,),
            in_specs=[pl.BlockSpec((rows, columns), head)],
            out_specs=pl.BlockSpec((1, rows, columns), lambda i, head_map: (i, 0, 0)),
        ),
        compiler_params=pltpu.CompilerParams(vmem_limit_bytes=4 * 1024 * 1024),
        name="pick",
    )(head_map, source_rows)
    gathered = pl.pallas_call(
        functools.partial(gather_kernel, n, tp),
        out_shape=jax.ShapeDtypeStruct((n, slots, rows, columns), source_rows.dtype),
        in_specs=[pl.BlockSpec(memory_space=pl.ANY)],
        out_specs=pl.BlockSpec(memory_space=pl.ANY),
        scratch_shapes=[pltpu.VMEM((n, rows, columns), source_rows.dtype)]
        + [pltpu.SemaphoreType.DMA((2, CHUNKS))] * 2
        + [pltpu.SemaphoreType.DMA((n - 1, 2, 2 * CHUNKS))] * 2
        + [pltpu.SemaphoreType.DMA((n - 1, 2, CHUNKS))] * 2
        + [pltpu.SemaphoreType.DMA((2, CHUNKS))] * 2,
        compiler_params=pltpu.CompilerParams(
            collective_id=0, has_side_effects=True, vmem_limit_bytes=8 * 1024 * 1024
        ),
        name="gather",
    )(pieces)
    together = max(1, 128 // rows)
    if together == 1:
        order = span_order
        reads, writes = [lambda p, order: (p, 0, 0, 0)], lambda p, order: (0, order[p])
    else:
        order = invert_order(span_order)
        reads = [
            functools.partial(lambda j, p, order: (order[p * together + j], 0, 0, 0), j)
            for j in range(together)
        ]
        writes = lambda p, order: (0, p)
    packed = pl.pallas_call(
        pack_kernel,
        out_shape=jax.ShapeDtypeStruct((slots * columns, n * rows), jnp.float32),
        grid_spec=pltpu.PrefetchScalarGridSpec(
            num_scalar_prefetch=1,
            grid=(n // together,),
            in_specs=[pl.BlockSpec((1, slots, rows, columns), read) for read in reads],
            out_specs=pl.BlockSpec((slots * columns, together * rows), writes),
        ),
        compiler_params=pltpu.CompilerParams(vmem_limit_bytes=16 * 1024 * 1024),
        name="pack",
    )(order, *[gathered] * together)
    return packed


def solution(mesh):
    n, tp = mesh.shape["grp"], mesh.shape["tp"]
    placed = (P("grp", "tp"), P(), P())
    return jax.shard_map(
        functools.partial(local, n, tp), mesh=mesh, in_specs=placed,
        out_specs=P("tp", None), check_vma=False,
    )
```

```python
import functools

import jax
import jax.numpy as jnp
from jax import lax
from jax.experimental import pallas as pl
from jax.experimental.pallas import tpu as pltpu
from jax.sharding import PartitionSpec as P

MESH = pl.DeviceIdType.MESH
CHUNKS = 2


def ring_member(position, n):
    half = position // (n // 2)
    return 2 * position * (1 - half) + (2 * (n - 1 - position) + 1) * half


def ring_position(member, n):
    odd = member % 2
    return (member // 2) * (1 - odd) + (n - 1 - member // 2) * odd


def gather_kernel(n, tp, slots, source, head_map, gathered, block, heads, pieces, carried, load, x_send, x_recv, r_send, r_recv, d_send, d_recv, o_send, o_recv):
    loads = [
        pltpu.make_async_copy(head_map, heads, load.at[0]),
        pltpu.make_async_copy(source, block, load.at[1]),
    ]
    for copy in loads:
        copy.start()
    rows = pieces.shape[1]
    me, k = lax.axis_index("grp"), lax.axis_index("tp")
    position = ring_position(me, n)
    ring = [ring_member((position + 1) % n, n), ring_member((position + n - 1) % n, n)]
    size = rows // (2 * CHUNKS)
    every = [(c, way) for c in range(CHUNKS) for way in range(2)]
    served = [(k + 2 * tp - tp // 2 - i) % tp for i in range(2)]

    barrier = pltpu.get_barrier_semaphore()
    for step in range(1, tp):
        pl.semaphore_signal(barrier, inc=1, device_id=(me, (k + step) % tp), device_id_type=MESH)
    for other in ring:
        pl.semaphore_signal(barrier, inc=1, device_id=(other, k), device_id_type=MESH)
    for copy in loads:
        copy.wait()
    columns = pieces.shape[2]
    for i in range(slots):
        head = heads[served[i] * slots + i] - k * slots
        chosen = block[:, :columns]
        for j in range(1, slots):
            chosen = jnp.where(head == j, block[:, j * columns:(j + 1) * columns], chosen)
        pieces[i] = chosen
    pl.semaphore_wait(barrier, tp + 1)

    def span(c, way):
        return pl.ds((way * CHUNKS + c) * size, size)

    def send(src, dst, send_sem, recv_sem, to):
        return pltpu.make_async_remote_copy(
            src_ref=src, dst_ref=dst, send_sem=send_sem, recv_sem=recv_sem,
            device_id=to, device_id_type=MESH,
        )

    def held(step, way):
        return ring_member((position + (n - step if way == 0 else step)) % n, n)

    def exchange(c, way):
        return send(pieces.at[0, span(c, way)], gathered.at[me, 0, span(c, way)],
                    x_send.at[way, c], x_recv.at[way, c], (me, served[0]))

    def own(c, way):
        return send(pieces.at[1, span(c, way)], gathered.at[me, 1, span(c, way)],
                    o_send.at[way, c], o_recv.at[way, c], (me, served[1]))

    def hop(step, c, way):
        chunk = gathered.at[held(step, way), 0, span(c, way)]
        return send(chunk, chunk, r_send.at[step, way, c], r_recv.at[step, way, c], (ring[way], k))

    def first(c, way):
        return send(pieces.at[1, span(c, way)], carried.at[me, span(c, way)],
                    r_send.at[0, way, CHUNKS + c], r_recv.at[0, way, CHUNKS + c], (ring[way], k))

    def carry(step, c, way):
        chunk = carried.at[held(step, way), span(c, way)]
        return send(chunk, chunk, r_send.at[step, way, CHUNKS + c], r_recv.at[step, way, CHUNKS + c],
                    (ring[way], k))

    def hand(step, c, way):
        owner = held(step, way)
        return send(carried.at[owner, span(c, way)], gathered.at[owner, 1, span(c, way)],
                    d_send.at[step - 1, way, c], d_recv.at[step - 1, way, c], (me, served[1]))

    for c, way in every:
        exchange(c, way).start()
    for c, way in every:
        first(c, way).start()
    both = range(2)
    for c in range(CHUNKS):
        for way in both:
            exchange(c, way).wait_recv()
            hop(0, c, way).start()
        for way in both:
            carry(0, c, way).wait_recv()
            carry(1, c, way).start()
    for c, way in every:
        own(c, way).start()
        hand(1, c, way).start()

    def forward(step, _):
        for c in range(CHUNKS):
            for way in both:
                hop(step - 1, c, way).wait_recv()
                hop(step, c, way).start()
            for way in both:
                carry(step, c, way).wait_recv()
                carry(step + 1, c, way).start()
                hand(step + 1, c, way).start()
        return _

    lax.fori_loop(1, n - 2, forward, 0)
    for c in range(CHUNKS):
        for way in both:
            hop(n - 3, c, way).wait_recv()
            hop(n - 2, c, way).start()
        for way in both:
            carry(n - 2, c, way).wait_recv()
            hand(n - 1, c, way).start()
    for c, way in every:
        own(c, way).wait()
        exchange(c, way).wait_send()

    def drain(step, _):
        for c, way in every:
            hop(step, c, way).wait_send()
            carry(step, c, way).wait_send()
            hand(step + 1, c, way).wait()
        return _

    lax.fori_loop(0, n - 2, drain, 0)
    for c, way in every:
        hop(n - 2, c, way).wait_recv()
    drain(n - 2, 0)


def place_kernel(order, gathered, out, order_here, ready, load, sems):
    n, slots, rows, columns = gathered.shape
    width = columns // 2
    fetch = pltpu.make_async_copy(order, order_here, load)
    fetch.start()
    copies = []
    for p in range(n):
        for c in range(2):
            for i in range(slots):
                cut = gathered[p, i, :, c * width:(c + 1) * width]
                ready[p, pl.ds((c * slots + i) * width, width), :] = cut.T.astype(jnp.float32)
        if p == 0:
            fetch.wait()
        start = pl.multiple_of(order_here[p] * rows, 128)
        copies.append(pltpu.make_async_copy(ready.at[p], out.at[:, pl.ds(start, rows)], sems.at[p]))
        copies[-1].start()
    for copy in copies:
        copy.wait()


def pack_kernel(order, *refs):
    blocks, out = refs[:-1], refs[-1]
    slots, width = blocks[0].shape[1], blocks[0].shape[3] // 2
    for c in range(2):
        for i in range(slots):
            cut = [b[0, i, :, c * width:(c + 1) * width] for b in blocks]
            whole = cut[0] if len(cut) == 1 else jnp.concatenate(cut, axis=0)
            out[pl.ds((c * slots + i) * width, width), :] = whole.T.astype(jnp.float32)


def invert_order(span_order):
    block_count = span_order.shape[0]
    positions = jnp.arange(block_count, dtype=jnp.int32)
    matches = (span_order[:, None] == positions[None, :]).astype(jnp.int32)
    return jnp.sum(matches * positions[:, None], axis=0)


def local(n, tp, source_rows, span_order, head_map):
    rows = source_rows.shape[0]
    slots = head_map.shape[0] // tp
    columns = source_rows.shape[1] // slots
    dtype = source_rows.dtype
    sems = pltpu.SemaphoreType.DMA
    gathered = pl.pallas_call(
        functools.partial(gather_kernel, n, tp, slots),
        out_shape=jax.ShapeDtypeStruct((n, slots, rows, columns), dtype),
        in_specs=[pl.BlockSpec(memory_space=pltpu.HBM)] * 2,
        out_specs=pl.BlockSpec(memory_space=pl.ANY),
        scratch_shapes=[
            pltpu.VMEM(source_rows.shape, dtype),
            pltpu.SMEM(head_map.shape, head_map.dtype),
            pltpu.VMEM((slots, rows, columns), dtype),
            pltpu.VMEM((n, rows, columns), dtype),
            sems((2,)),
        ]
        + [sems((2, CHUNKS))] * 2
        + [sems((n - 1, 2, 2 * CHUNKS))] * 2
        + [sems((n - 1, 2, CHUNKS))] * 2
        + [sems((2, CHUNKS))] * 2,
        compiler_params=pltpu.CompilerParams(
            collective_id=0, has_side_effects=True, vmem_limit_bytes=8 * 1024 * 1024
        ),
        name="gather",
    )(*[pltpu.with_memory_space_constraint(a, pltpu.HBM) for a in (source_rows, head_map)])
    if rows % 128 == 0:
        return pl.pallas_call(
            place_kernel,
            out_shape=jax.ShapeDtypeStruct((slots * columns, n * rows), jnp.float32),
            in_specs=[pl.BlockSpec(memory_space=pltpu.HBM), pl.BlockSpec(memory_space=pltpu.VMEM)],
            out_specs=pl.BlockSpec(memory_space=pltpu.HBM),
            scratch_shapes=[
                pltpu.SMEM(span_order.shape, span_order.dtype),
                pltpu.VMEM((n, slots * columns, rows), jnp.float32),
                pltpu.SemaphoreType.DMA,
                sems((n,)),
            ],
            compiler_params=pltpu.CompilerParams(vmem_limit_bytes=24 * 1024 * 1024),
            name="place",
        )(pltpu.with_memory_space_constraint(span_order, pltpu.HBM), gathered)
    together = max(1, 128 // rows)
    inverse = invert_order(span_order)
    reads = [
        functools.partial(lambda j, b, order: (order[b * together + j], 0, 0, 0), j)
        for j in range(together)
    ]
    packed = pl.pallas_call(
        pack_kernel,
        out_shape=jax.ShapeDtypeStruct((slots * columns, n * rows), jnp.float32),
        grid_spec=pltpu.PrefetchScalarGridSpec(
            num_scalar_prefetch=1,
            grid=(n // together,),
            in_specs=[pl.BlockSpec((1, slots, rows, columns), read) for read in reads],
            out_specs=pl.BlockSpec((slots * columns, together * rows), lambda b, order: (0, b)),
        ),
        compiler_params=pltpu.CompilerParams(vmem_limit_bytes=16 * 1024 * 1024),
        name="pack",
    )(inverse, *[gathered] * together)
    return packed


def solution(mesh):
    n, tp = mesh.shape["grp"], mesh.shape["tp"]
    placed = (P("grp", "tp"), P(), P())
    return jax.shard_map(
        functools.partial(local, n, tp), mesh=mesh, in_specs=placed,
        out_specs=P("tp", None), check_vma=False,
    )
```

```python
import functools

import jax
import jax.numpy as jnp
from jax import lax
from jax.experimental import pallas as pl
from jax.experimental.pallas import tpu as pltpu
from jax.sharding import PartitionSpec as P

MESH = pl.DeviceIdType.MESH
CHUNKS = 2


def ring_member(position, n):
    half = position // (n // 2)
    return 2 * position * (1 - half) + (2 * (n - 1 - position) + 1) * half


def ring_position(member, n):
    odd = member % 2
    return (member // 2) * (1 - odd) + (n - 1 - member // 2) * odd


def gather_kernel(n, tp, slots, source, head_map, gathered, block, heads, pieces, carried, load, x_send, x_recv, r_send, r_recv, d_send, d_recv, o_send, o_recv):
    loads = [
        pltpu.make_async_copy(head_map, heads, load.at[0]),
        pltpu.make_async_copy(source, block, load.at[1]),
    ]
    for copy in loads:
        copy.start()
    rows = pieces.shape[1]
    me, k = lax.axis_index("grp"), lax.axis_index("tp")
    position = ring_position(me, n)
    ring = [ring_member((position + 1) % n, n), ring_member((position + n - 1) % n, n)]
    size = rows // (2 * CHUNKS)
    every = [(c, way) for c in range(CHUNKS) for way in range(2)]
    served = [(k + 2 * tp - tp // 2 - i) % tp for i in range(2)]

    barrier = pltpu.get_barrier_semaphore()
    for step in range(1, tp):
        pl.semaphore_signal(barrier, inc=1, device_id=(me, (k + step) % tp), device_id_type=MESH)
    for other in ring:
        pl.semaphore_signal(barrier, inc=1, device_id=(other, k), device_id_type=MESH)
    for copy in loads:
        copy.wait()
    columns = pieces.shape[2]
    for i in range(slots):
        head = heads[served[i] * slots + i] - k * slots
        chosen = block[:, :columns]
        for j in range(1, slots):
            chosen = jnp.where(head == j, block[:, j * columns:(j + 1) * columns], chosen)
        pieces[i] = chosen
    pl.semaphore_wait(barrier, tp + 1)

    def span(c, way):
        return pl.ds((way * CHUNKS + c) * size, size)

    def send(src, dst, send_sem, recv_sem, to):
        return pltpu.make_async_remote_copy(
            src_ref=src, dst_ref=dst, send_sem=send_sem, recv_sem=recv_sem,
            device_id=to, device_id_type=MESH,
        )

    def held(step, way):
        return ring_member((position + (n - step if way == 0 else step)) % n, n)

    def exchange(c, way):
        return send(pieces.at[0, span(c, way)], gathered.at[me, 0, span(c, way)],
                    x_send.at[way, c], x_recv.at[way, c], (me, served[0]))

    def own(c, way):
        return send(pieces.at[1, span(c, way)], gathered.at[me, 1, span(c, way)],
                    o_send.at[way, c], o_recv.at[way, c], (me, served[1]))

    def hop(step, c, way):
        chunk = gathered.at[held(step, way), 0, span(c, way)]
        return send(chunk, chunk, r_send.at[step, way, c], r_recv.at[step, way, c], (ring[way], k))

    def first(c, way):
        return send(pieces.at[1, span(c, way)], carried.at[me, span(c, way)],
                    r_send.at[0, way, CHUNKS + c], r_recv.at[0, way, CHUNKS + c], (ring[way], k))

    def carry(step, c, way):
        chunk = carried.at[held(step, way), span(c, way)]
        return send(chunk, chunk, r_send.at[step, way, CHUNKS + c], r_recv.at[step, way, CHUNKS + c],
                    (ring[way], k))

    def hand(step, c, way):
        owner = held(step, way)
        return send(carried.at[owner, span(c, way)], gathered.at[owner, 1, span(c, way)],
                    d_send.at[step - 1, way, c], d_recv.at[step - 1, way, c], (me, served[1]))

    for c, way in every:
        exchange(c, way).start()
    for c, way in every:
        first(c, way).start()
    both = range(2)
    for c in range(CHUNKS):
        for way in both:
            exchange(c, way).wait_recv()
            hop(0, c, way).start()
        for way in both:
            carry(0, c, way).wait_recv()
            carry(1, c, way).start()
    for c, way in every:
        own(c, way).start()
        hand(1, c, way).start()

    def forward(step, _):
        for c in range(CHUNKS):
            for way in both:
                hop(step - 1, c, way).wait_recv()
                hop(step, c, way).start()
            for way in both:
                carry(step, c, way).wait_recv()
                carry(step + 1, c, way).start()
                hand(step + 1, c, way).start()
        return _

    lax.fori_loop(1, n - 2, forward, 0)
    for c in range(CHUNKS):
        for way in both:
            hop(n - 3, c, way).wait_recv()
            hop(n - 2, c, way).start()
        for way in both:
            carry(n - 2, c, way).wait_recv()
            hand(n - 1, c, way).start()
    for c, way in every:
        own(c, way).wait()
        exchange(c, way).wait_send()

    def drain(step, _):
        for c, way in every:
            hop(step, c, way).wait_send()
            carry(step, c, way).wait_send()
            hand(step + 1, c, way).wait()
        return _

    lax.fori_loop(0, n - 2, drain, 0)
    for c, way in every:
        hop(n - 2, c, way).wait_recv()
    drain(n - 2, 0)


def place_kernel(order, gathered, out, order_here, ready, load, sems):
    n, slots, rows, columns = gathered.shape
    width = columns // 2
    fetch = pltpu.make_async_copy(order, order_here, load)
    fetch.start()
    copies = []
    half = slots * width
    for p in range(n):
        for c in range(2):
            for i in range(slots):
                cut = gathered[p, i, :, c * width:(c + 1) * width]
                ready[p, pl.ds((c * slots + i) * width, width), :] = cut.T.astype(jnp.float32)
            if p == 0 and c == 0:
                fetch.wait()
            start = pl.multiple_of(order_here[p] * rows, 128)
            copies.append(pltpu.make_async_copy(
                ready.at[p, pl.ds(c * half, half)],
                out.at[pl.ds(c * half, half), pl.ds(start, rows)],
                sems.at[p, c],
            ))
            copies[-1].start()
    for copy in copies:
        copy.wait()


def pack_kernel(order, *refs):
    blocks, out = refs[:-1], refs[-1]
    slots, width = blocks[0].shape[1], blocks[0].shape[3] // 2
    for c in range(2):
        for i in range(slots):
            cut = [b[0, i, :, c * width:(c + 1) * width] for b in blocks]
            whole = cut[0] if len(cut) == 1 else jnp.concatenate(cut, axis=0)
            out[pl.ds((c * slots + i) * width, width), :] = whole.T.astype(jnp.float32)


def invert_order(span_order):
    block_count = span_order.shape[0]
    positions = jnp.arange(block_count, dtype=jnp.int32)
    matches = (span_order[:, None] == positions[None, :]).astype(jnp.int32)
    return jnp.sum(matches * positions[:, None], axis=0)


def local(n, tp, source_rows, span_order, head_map):
    rows = source_rows.shape[0]
    slots = head_map.shape[0] // tp
    columns = source_rows.shape[1] // slots
    dtype = source_rows.dtype
    sems = pltpu.SemaphoreType.DMA
    gathered = pl.pallas_call(
        functools.partial(gather_kernel, n, tp, slots),
        out_shape=jax.ShapeDtypeStruct((n, slots, rows, columns), dtype),
        in_specs=[pl.BlockSpec(memory_space=pltpu.HBM)] * 2,
        out_specs=pl.BlockSpec(memory_space=pl.ANY),
        scratch_shapes=[
            pltpu.VMEM(source_rows.shape, dtype),
            pltpu.SMEM(head_map.shape, head_map.dtype),
            pltpu.VMEM((slots, rows, columns), dtype),
            pltpu.VMEM((n, rows, columns), dtype),
            sems((2,)),
        ]
        + [sems((2, CHUNKS))] * 2
        + [sems((n - 1, 2, 2 * CHUNKS))] * 2
        + [sems((n - 1, 2, CHUNKS))] * 2
        + [sems((2, CHUNKS))] * 2,
        compiler_params=pltpu.CompilerParams(
            collective_id=0, has_side_effects=True, vmem_limit_bytes=8 * 1024 * 1024
        ),
        name="gather",
    )(*[pltpu.with_memory_space_constraint(a, pltpu.HBM) for a in (source_rows, head_map)])
    if rows % 128 == 0:
        return pl.pallas_call(
            place_kernel,
            out_shape=jax.ShapeDtypeStruct((slots * columns, n * rows), jnp.float32),
            in_specs=[pl.BlockSpec(memory_space=pltpu.HBM), pl.BlockSpec(memory_space=pltpu.VMEM)],
            out_specs=pl.BlockSpec(memory_space=pltpu.HBM),
            scratch_shapes=[
                pltpu.SMEM(span_order.shape, span_order.dtype),
                pltpu.VMEM((n, slots * columns, rows), jnp.float32),
                pltpu.SemaphoreType.DMA,
                sems((n, 2)),
            ],
            compiler_params=pltpu.CompilerParams(vmem_limit_bytes=24 * 1024 * 1024),
            name="place",
        )(pltpu.with_memory_space_constraint(span_order, pltpu.HBM), gathered)
    together = max(1, 128 // rows)
    inverse = invert_order(span_order)
    reads = [
        functools.partial(lambda j, b, order: (order[b * together + j], 0, 0, 0), j)
        for j in range(together)
    ]
    packed = pl.pallas_call(
        pack_kernel,
        out_shape=jax.ShapeDtypeStruct((slots * columns, n * rows), jnp.float32),
        grid_spec=pltpu.PrefetchScalarGridSpec(
            num_scalar_prefetch=1,
            grid=(n // together,),
            in_specs=[pl.BlockSpec((1, slots, rows, columns), read) for read in reads],
            out_specs=pl.BlockSpec((slots * columns, together * rows), lambda b, order: (0, b)),
        ),
        compiler_params=pltpu.CompilerParams(vmem_limit_bytes=16 * 1024 * 1024),
        name="pack",
    )(inverse, *[gathered] * together)
    return packed


def solution(mesh):
    n, tp = mesh.shape["grp"], mesh.shape["tp"]
    placed = (P("grp", "tp"), P(), P())
    return jax.shard_map(
        functools.partial(local, n, tp), mesh=mesh, in_specs=placed,
        out_specs=P("tp", None), check_vma=False,
    )
```
